32 devices in a mesh: grp: 2 (over y), seq: 16 (over z, x, core).
Axes of the slice: x: 2, y: 2, z: 4, core: 2. Of those that a mesh axis runs over, the one named last changes fastest.
Arguments:
- queries: bfloat16 [4096, 12288], P(('grp', 'seq')), parts along dimension 0, may hold values from -8 to 8
- sum_keys: bfloat16 [256, 768], P(('grp', 'seq')), parts along dimension 0, may hold values from -4 to 4
- sum_values: bfloat16 [256, 512], P(('grp', 'seq')), parts along dimension 0, may hold values from -24 to 24
- limits: int32 [64], P('grp'), parts along dimension 0, may hold values from 1 to 128, as said below
- valid_tokens: int32 [2], P('grp'), parts along dimension 0, may hold values from 1024 to 2048
Outputs:
- attended: bfloat16 [4096, 8192], P(('grp', 'seq')), parts along dimension 0
The draws below stay inside these ranges and needn't reach their ends.
There are 2 independent parts, one for each index of `grp`. The reference program is written for one: setup_inputs(seed, part) draws one part's arguments, and reference() takes and returns one part's arrays. A program takes and returns all parts, laid end to end along the dimension named above; each array names one. Nothing has to cross between parts.
Inputs may be any that keep to these rules, and one draw needn't show every extreme that they name: limits[b] is at least 1 and at most max(1, (64 * b - 32) // 16 + 1), the number of summaries that end at or before the block's first token; the last block reaches this bound.
All inputs are finite; a program needn't handle non-finite values.
Results may differ from the reference program's by a relative error of at most 0.0027.
Values may be sent and summed in bfloat16 or wider, within the bound.
A program may use at most 64 MiB of HBM per device.

```python
import jax
import jax.numpy as jnp
from jax import lax

H = 64
G = 4
DK = 192
DV = 128
STRIDE = 16
CBLOCK = 32
QB = 64
L = 2048
NS = 128
NB = 32


def summary_key_law(key):
    inner = jax.random.fold_in(key, 11)
    values = jnp.clip(jax.random.normal(inner, (NS, G * DK)), -4.0, 4.0)
    return values.astype(jnp.float32)


def draw_sum_keys(key, part):
    return summary_key_law(key).astype(jnp.bfloat16)


def draw_queries(key, part):
    inner = jax.random.fold_in(key, 23)
    values = jnp.clip(2.5 * jax.random.normal(inner, (L, H * DK)), -8.0, 8.0)
    return values.astype(jnp.bfloat16)


def draw_limits(key, part):
    block_ids = jnp.arange(NB, dtype=jnp.int32)
    causal = jnp.maximum((QB * block_ids - CBLOCK) // STRIDE + 1, 1).astype(jnp.int32)
    offsets = jax.random.randint(jax.random.fold_in(key, 5), (NB,), 0, 1 << 20, dtype=jnp.int32) % (causal // 4 + 1)
    drawn = causal - offsets
    return drawn.at[NB - 1].set(causal[NB - 1]).astype(jnp.int32)


def shard_levels(stream_key, dims, pieces, smallest, high):
    def one(dim, parts):
        heights = jax.random.uniform(jax.random.fold_in(jax.random.fold_in(stream_key, 6), dim), (parts,), jnp.float32, smallest / len(pieces), high / len(pieces))
        return jnp.repeat(jnp.exp(heights), dims[dim] // parts).reshape((-1,) + (1,) * (len(dims) - dim - 1))

    loudness = one(*pieces[0])
    for cut in pieces[1:]:
        loudness = loudness * one(*cut)
    return loudness


def scatter_about(own_key, extent, scale, most, cuts=(), kind=jnp.bfloat16):
    gain = shard_levels(own_key, extent, cuts, -0.22, 0.18) if cuts else 1.0
    result = jax.random.normal(own_key, extent, jnp.float32) * scale * gain
    return jnp.minimum(jnp.maximum(result, -most), most).astype(kind)


def setup_inputs(seed: int = 0, part: int = 0) -> dict:
    splits = jax.random.split(jax.random.key(seed), 6)
    part_splits = jax.random.split(jax.random.fold_in(splits[5], part), 6)
    return {
        "queries": draw_queries(jax.random.fold_in(jax.random.fold_in(splits[5], part), 71), part),
        "sum_keys": draw_sum_keys(jax.random.fold_in(jax.random.fold_in(splits[5], part), 71), part),
        "sum_values": scatter_about(part_splits[2], (NS, G * DV), 4.0, 24.0, ((0, 16),)),
        "limits": draw_limits(jax.random.fold_in(jax.random.fold_in(splits[5], part), 71), part),
        "valid_tokens": jax.random.randint(part_splits[4], (1,), L // 2, L + 1).astype(jnp.int32),
    }


def reference(queries, sum_keys, sum_values, limits, valid_tokens):
    per_group = H // G
    inv_root = float(DK) ** -0.5
    usable = jnp.maximum((valid_tokens[0] - CBLOCK) // STRIDE + 1, 1).astype(jnp.int32)
    key_table = sum_keys.reshape(NS, G, DK).astype(jnp.float32)
    value_table = sum_values.reshape(NS, G, DV).astype(jnp.float32)
    summary_ids = jnp.arange(NS, dtype=jnp.int32)

    def one_block(block_args):
        query_block, block_limit = block_args
        grouped = query_block.reshape(QB, G, per_group, DK).astype(jnp.float32)
        scores = jnp.einsum("tgjd,sgd->tgjs", grouped, key_table, precision=lax.Precision.HIGHEST) * inv_root
        visible = summary_ids < jnp.minimum(block_limit, usable)
        scores = jnp.where(visible, scores, -1e30)
        row_max = jnp.max(scores, axis=-1, keepdims=True)
        weights = jnp.where(visible, jnp.exp(scores - row_max), 0.0)
        row_total = jnp.sum(weights, axis=-1, keepdims=True)
        rounded = lax.optimization_barrier(weights.astype(jnp.bfloat16)).astype(jnp.float32)
        blended = jnp.einsum("tgjs,sgd->tgjd", rounded, value_table, precision=lax.Precision.HIGHEST) / row_total
        return blended.reshape(QB, H * DV).astype(jnp.bfloat16)

    blocks = lax.map(one_block, (queries.reshape(NB, QB, H * DK), limits))
    return blocks.reshape(L, H * DV)
```

```python
import functools

import jax
import jax.numpy as jnp
from jax import lax
from jax.experimental import pallas as pl
from jax.experimental.pallas import tpu as pltpu
from jax.sharding import PartitionSpec as P

H = 64
G = 4
DK = 192
DV = 128
STRIDE = 16
CBLOCK = 32
QB = 64
LOG2E = 1.4426950408889634
MESH = pl.DeviceIdType.MESH


def gather_kernel(n, keys_hbm, values_hbm, q_hbm, kv_ref, q_ref, in_sem, q_sem, send_sem, plane_sem, recv_sem):
    me = lax.axis_index("seq")
    depth = n // 4
    outer = me // 4
    lane = me % 4
    kw = keys_hbm.shape[1]
    load_k = pltpu.make_async_copy(keys_hbm, kv_ref.at[me, :, pl.ds(0, kw)], in_sem.at[0])
    load_v = pltpu.make_async_copy(values_hbm, kv_ref.at[me, :, pl.ds(kw, values_hbm.shape[1])], in_sem.at[1])
    load_k.start()
    load_v.start()
    load_q = pltpu.make_async_copy(q_hbm, q_ref, q_sem)
    load_q.start()

    barrier = pltpu.get_barrier_semaphore()
    for step in range(1, depth):
        @pl.when(outer >= step)
        def _():
            pl.semaphore_signal(barrier, inc=1, device_id={"seq": me - 4 * step}, device_id_type=MESH)
    for step in range(1, 4):
        pl.semaphore_signal(barrier, inc=1, device_id={"seq": outer * 4 + (lane + step) % 4}, device_id_type=MESH)
    load_k.wait()
    load_v.wait()
    pl.semaphore_wait(barrier, depth - 1 - outer + 3)

    def up(step):
        return pltpu.make_async_remote_copy(
            src_ref=kv_ref.at[me],
            dst_ref=kv_ref.at[me],
            send_sem=send_sem.at[step],
            recv_sem=recv_sem.at[me],
            device_id={"seq": me + 4 * step},
            device_id_type=MESH,
        )

    def across(level, step):
        slot = level * 4 + lane
        return pltpu.make_async_remote_copy(
            src_ref=kv_ref.at[slot],
            dst_ref=kv_ref.at[slot],
            send_sem=plane_sem.at[level * 3 + step - 1],
            recv_sem=recv_sem.at[slot],
            device_id={"seq": outer * 4 + (lane + step) % 4},
            device_id_type=MESH,
        )

    def arrived(slot):
        pltpu.make_async_copy(kv_ref.at[slot], kv_ref.at[slot], recv_sem.at[slot]).wait()

    for step in range(depth - 1, 0, -1):
        @pl.when(outer + step < depth)
        def _():
            up(step).start()
    for step in range(1, 4):
        across(outer, step).start()
    for back in range(1, depth):
        @pl.when(outer >= back)
        def _():
            arrived((outer - back) * 4 + lane)
            for step in range(1, 4):
                across(outer - back, step).start()
    for level in range(depth):
        @pl.when(level > outer)
        def _():
            kv_ref[pl.ds(level * 4, 4)] = jnp.zeros((4,) + kv_ref.shape[1:], kv_ref.dtype)
    for level in range(depth):
        @pl.when(level <= outer)
        def _():
            for step in range(1, 4):
                arrived(level * 4 + (lane + step) % 4)
    for step in range(1, depth):
        @pl.when(outer + step < depth)
        def _():
            up(step).wait_send()
    for level in range(depth):
        @pl.when(level <= outer)
        def _():
            for step in range(1, 4):
                across(level, step).wait_send()
    load_q.wait()


def attend_kernel(q_ref, kv_ref, limits_ref, valid_ref, out_hbm, keys_ref, values_ref, bias_ref, out_ref, out_sem):
    n, rows, _ = kv_ref.shape
    total = n * rows
    tokens = q_ref.shape[0]
    pairs = H // G // 2
    me = lax.axis_index("seq")
    usable = jnp.maximum((valid_ref[0] - CBLOCK) // STRIDE + 1, 1)
    ids = lax.broadcasted_iota(jnp.int32, (QB, total), 1)
    for block in range(tokens // QB):
        cap = jnp.minimum(limits_ref[me * (tokens // QB) + block], usable)
        bias_ref[block * QB:(block + 1) * QB, :] = jnp.where(ids < cap, 0.0, -1e30)

    col = lax.broadcasted_iota(jnp.int32, (total, 256), 1)
    for g in range(G):
        if g % 2 == 0:
            start = g * DK
            window = kv_ref[:, :, start:start + 256].astype(jnp.float32).reshape(total, 256)
            even = jnp.where(col < DK, window, 0.0)
            odd = pltpu.roll(even, 64, 1)
        else:
            start = g * DK - 64
            window = kv_ref[:, :, start:start + 256].astype(jnp.float32).reshape(total, 256)
            odd = jnp.where(col >= 64, window, 0.0)
            even = pltpu.roll(odd, 192, 1)
        keys_ref[g, 0] = even.astype(jnp.bfloat16)
        keys_ref[g, 1] = odd.astype(jnp.bfloat16)
        start = G * DK + g * DV
        value = kv_ref[:, :, start:start + DV].astype(jnp.float32).reshape(total, DV).astype(jnp.bfloat16)
        zero = jnp.zeros((total, DV), jnp.bfloat16)
        values_ref[g, 0:total, 0:DV] = value
        values_ref[g, 0:total, DV:2 * DV] = zero
        values_ref[g, total:2 * total, 0:DV] = zero
        values_ref[g, total:2 * total, DV:2 * DV] = value

    scale = float(DK) ** -0.5 * LOG2E
    nt = (((1,), (1,)), ((), ()))
    out_cols = pairs * 2 * DV

    def put(g):
        cols = pl.ds(pl.multiple_of(g * out_cols, 128), out_cols)
        return pltpu.make_async_copy(out_ref.at[:, cols], out_hbm.at[:, cols], out_sem.at[g])

    def one_group(g, _):
        for p in range(pairs):
            q_at = pl.multiple_of(g * (pairs * 2 * DK) + p * 2 * DK, 128)
            weights, norms = [], []
            for half in range(2):
                q = q_ref[:, pl.ds(q_at + half * 128, 256)]
                s = lax.dot_general(q, keys_ref[g, half], nt, preferred_element_type=jnp.float32)
                s = s + bias_ref[...]
                w = jnp.exp2((s - jnp.max(s, axis=1, keepdims=True)) * scale)
                norms.append(jnp.sum(w, axis=1, keepdims=True))
                weights.append(w.astype(jnp.bfloat16))
            both = jnp.concatenate(weights, axis=1)
            blended = jnp.dot(both, values_ref[g], preferred_element_type=jnp.float32)
            out_at = pl.multiple_of(g * out_cols + p * 2 * DV, 128)
            for half in range(2):
                out_ref[:, pl.ds(out_at + half * DV, DV)] = (
                    blended[:, half * DV:(half + 1) * DV] / norms[half]
                ).astype(jnp.bfloat16)
        put(g).start()
        return 0

    lax.fori_loop(0, G, one_group, 0)
    for g in range(G):
        put(g).wait()


def solution(mesh):
    n = mesh.shape["seq"]

    def per_device(queries, sum_keys, sum_values, limits, valid_tokens):
        rows = sum_keys.shape[0]
        tokens = queries.shape[0]
        width = sum_keys.shape[1] + sum_values.shape[1]
        total = n * rows
        hbm = pl.BlockSpec(memory_space=pl.ANY)
        vmem = pl.BlockSpec(memory_space=pltpu.VMEM)
        smem = pl.BlockSpec(memory_space=pltpu.SMEM)
        kv, q = pl.pallas_call(
            functools.partial(gather_kernel, n),
            out_shape=(
                pltpu.VMEM((n, rows, width), jnp.bfloat16),
                pltpu.VMEM(queries.shape, jnp.bfloat16),
            ),
            in_specs=[hbm, hbm, hbm],
            out_specs=(vmem, vmem),
            scratch_shapes=[
                pltpu.SemaphoreType.DMA((2,)),
                pltpu.SemaphoreType.DMA,
                pltpu.SemaphoreType.DMA((n // 4,)),
                pltpu.SemaphoreType.DMA((n // 4 * 3,)),
                pltpu.SemaphoreType.DMA((n,)),
            ],
            compiler_params=pltpu.CompilerParams(collective_id=0, has_side_effects=True, vmem_limit_bytes=16 * 1024 * 1024),
            name="gather",
        )(sum_keys, sum_values, queries)
        return pl.pallas_call(
            attend_kernel,
            out_shape=jax.ShapeDtypeStruct((tokens, H * DV), jnp.bfloat16),
            in_specs=[vmem, vmem, smem, smem],
            out_specs=hbm,
            scratch_shapes=[
                pltpu.VMEM((G, 2, total, 256), jnp.bfloat16),
                pltpu.VMEM((G, 2 * total, 2 * DV), jnp.bfloat16),
                pltpu.VMEM((tokens, total), jnp.float32),
                pltpu.VMEM((tokens, H * DV), jnp.bfloat16),
                pltpu.SemaphoreType.DMA((G,)),
            ],
            compiler_params=pltpu.CompilerParams(vmem_limit_bytes=40 * 1024 * 1024),
            name="attend",
        )(q, kv, limits, valid_tokens)

    placed = (
        P(("grp", "seq"), None),
        P(("grp", "seq"), None),
        P(("grp", "seq"), None),
        P("grp"),
        P("grp"),
    )
    return jax.shard_map(
        per_device, mesh=mesh, in_specs=placed, out_specs=P(("grp", "seq"), None), check_vma=False
    )
```

```python
import functools

import jax
import jax.numpy as jnp
from jax import lax
from jax.experimental import pallas as pl
from jax.experimental.pallas import tpu as pltpu
from jax.sharding import PartitionSpec as P

H = 64
G = 4
DK = 192
DV = 128
STRIDE = 16
CBLOCK = 32
QB = 64
LOG2E = 1.4426950408889634
MESH = pl.DeviceIdType.MESH


def gather_kernel(
    n, keys_hbm, values_hbm, q_hbm, limits_hbm, valid_hbm, kv_ref, q_ref, bias_ref,
    limits_ref, valid_ref, in_sem, q_sem, send_sem, plane_sem, recv_sem
):
    me = lax.axis_index("seq")
    depth = n // 4
    outer = me // 4
    lane = me % 4
    kw = keys_hbm.shape[1]
    load_k = pltpu.make_async_copy(keys_hbm, kv_ref.at[me, :, pl.ds(0, kw)], in_sem.at[0])
    load_v = pltpu.make_async_copy(values_hbm, kv_ref.at[me, :, pl.ds(kw, values_hbm.shape[1])], in_sem.at[1])
    load_k.start()
    load_v.start()
    load_q = pltpu.make_async_copy(q_hbm, q_ref, q_sem)
    load_q.start()
    load_limits = pltpu.make_async_copy(limits_hbm, limits_ref, in_sem.at[2])
    load_valid = pltpu.make_async_copy(valid_hbm, valid_ref, in_sem.at[3])
    load_limits.start()
    load_valid.start()

    barrier = pltpu.get_barrier_semaphore()
    for step in range(1, depth):
        @pl.when(outer >= step)
        def _():
            pl.semaphore_signal(barrier, inc=1, device_id={"seq": me - 4 * step}, device_id_type=MESH)
    for step in range(1, 4):
        pl.semaphore_signal(barrier, inc=1, device_id={"seq": outer * 4 + (lane + step) % 4}, device_id_type=MESH)
    load_k.wait()
    load_v.wait()
    pl.semaphore_wait(barrier, depth - 1 - outer + 3)

    def up(step):
        return pltpu.make_async_remote_copy(
            src_ref=kv_ref.at[me],
            dst_ref=kv_ref.at[me],
            send_sem=send_sem.at[step],
            recv_sem=recv_sem.at[me],
            device_id={"seq": me + 4 * step},
            device_id_type=MESH,
        )

    def across(level, step):
        slot = level * 4 + lane
        return pltpu.make_async_remote_copy(
            src_ref=kv_ref.at[slot],
            dst_ref=kv_ref.at[slot],
            send_sem=plane_sem.at[level * 3 + step - 1],
            recv_sem=recv_sem.at[slot],
            device_id={"seq": outer * 4 + (lane + step) % 4},
            device_id_type=MESH,
        )

    def arrived(slot):
        pltpu.make_async_copy(kv_ref.at[slot], kv_ref.at[slot], recv_sem.at[slot]).wait()

    for step in range(depth - 1, 0, -1):
        @pl.when(outer + step < depth)
        def _():
            up(step).start()
    for step in range(1, 4):
        across(outer, step).start()
    load_limits.wait()
    load_valid.wait()
    blocks, _, total = bias_ref.shape
    usable = jnp.maximum((valid_ref[0] - CBLOCK) // STRIDE + 1, 1)
    ids = lax.broadcasted_iota(jnp.int32, (8, total), 1)
    for block in range(blocks):
        cap = jnp.minimum(limits_ref[me * blocks + block], usable)
        bias_ref[block] = jnp.where(ids < cap, 0.0, -1e30)
    for back in range(1, depth):
        @pl.when(outer >= back)
        def _():
            arrived((outer - back) * 4 + lane)
            for step in range(1, 4):
                across(outer - back, step).start()
    for level in range(depth):
        @pl.when(level > outer)
        def _():
            kv_ref[pl.ds(level * 4, 4)] = jnp.zeros((4,) + kv_ref.shape[1:], kv_ref.dtype)
    for level in range(depth):
        @pl.when(level <= outer)
        def _():
            for step in range(1, 4):
                arrived(level * 4 + (lane + step) % 4)
    for step in range(1, depth):
        @pl.when(outer + step < depth)
        def _():
            up(step).wait_send()
    for level in range(depth):
        @pl.when(level <= outer)
        def _():
            for step in range(1, 4):
                across(level, step).wait_send()
    load_q.wait()


def attend_kernel(q_ref, kv_ref, bias_ref, out_hbm, keys_ref, values_ref, out_ref, s_ref, n_ref, w_ref, out_sem):
    n, rows, _ = kv_ref.shape
    total = n * rows
    tokens = q_ref.shape[0]
    pairs = H // G // 2

    col = lax.broadcasted_iota(jnp.int32, (total, 256), 1)
    for g in range(G):
        if g % 2 == 0:
            start = g * DK
            window = kv_ref[:, :, start:start + 256].astype(jnp.float32).reshape(total, 256)
            even = jnp.where(col < DK, window, 0.0)
            odd = pltpu.roll(even, 64, 1)
        else:
            start = g * DK - 64
            window = kv_ref[:, :, start:start + 256].astype(jnp.float32).reshape(total, 256)
            odd = jnp.where(col >= 64, window, 0.0)
            even = pltpu.roll(odd, 192, 1)
        keys_ref[g, 0] = even.astype(jnp.bfloat16)
        keys_ref[g, 1] = odd.astype(jnp.bfloat16)
        start = G * DK + g * DV
        value = kv_ref[:, :, start:start + DV].astype(jnp.float32).reshape(total, DV).astype(jnp.bfloat16)
        zero = jnp.zeros((total, DV), jnp.bfloat16)
        values_ref[g, 0:total, 0:DV] = value
        values_ref[g, 0:total, DV:2 * DV] = zero
        values_ref[g, total:2 * total, 0:DV] = zero
        values_ref[g, total:2 * total, DV:2 * DV] = value

    scale = float(DK) ** -0.5 * LOG2E
    nt = (((1,), (1,)), ((), ()))
    out_cols = pairs * 2 * DV

    def put(g):
        cols = pl.ds(pl.multiple_of(g * out_cols, 128), out_cols)
        return pltpu.make_async_copy(out_ref.at[:, cols], out_hbm.at[:, cols], out_sem.at[g])

    def one_group(g, _):
        base = pl.multiple_of(g * (pairs * 2 * DK), 128)
        for half in range(2):
            q = jnp.concatenate(
                [q_ref[:, pl.ds(base + p * 2 * DK + half * 128, 256)] for p in range(pairs)], axis=0
            )
            s_ref[half] = lax.dot_general(q, keys_ref[g, half], nt, preferred_element_type=jnp.float32)
        for p in range(pairs):
            for block in range(tokens // QB):
                at = slice(p * tokens + block * QB, p * tokens + (block + 1) * QB)
                bias = bias_ref[block, 0:1, :]
                for half in range(2):
                    s = s_ref[half, at, :] + bias
                    w = jnp.exp2((s - jnp.max(s, axis=1, keepdims=True)) * scale)
                    norm = jnp.sum(w, axis=1, keepdims=True)
                    n_ref[at, half * DV:(half + 1) * DV] = jnp.broadcast_to(1.0 / norm, (QB, DV))
                    w_ref[at, half * total:(half + 1) * total] = w.astype(jnp.bfloat16)
        blended = jnp.dot(w_ref[...], values_ref[g], preferred_element_type=jnp.float32) * n_ref[...]
        for p in range(pairs):
            out_at = pl.multiple_of(g * out_cols + p * 2 * DV, 128)
            out_ref[:, pl.ds(out_at, 2 * DV)] = blended[p * tokens:(p + 1) * tokens].astype(jnp.bfloat16)
        put(g).start()
        return 0

    lax.fori_loop(0, G, one_group, 0)
    for g in range(G):
        put(g).wait()


def solution(mesh):
    n = mesh.shape["seq"]

    def per_device(queries, sum_keys, sum_values, limits, valid_tokens):
        rows = sum_keys.shape[0]
        tokens = queries.shape[0]
        width = sum_keys.shape[1] + sum_values.shape[1]
        total = n * rows
        hbm = pl.BlockSpec(memory_space=pltpu.HBM)
        vmem = pl.BlockSpec(memory_space=pltpu.VMEM)
        kv, q, bias = pl.pallas_call(
            functools.partial(gather_kernel, n),
            out_shape=(
                pltpu.VMEM((n, rows, width), jnp.bfloat16),
                pltpu.VMEM(queries.shape, jnp.bfloat16),
                pltpu.VMEM((tokens // QB, 8, total), jnp.float32),
            ),
            in_specs=[hbm, hbm, hbm, hbm, hbm],
            out_specs=(vmem, vmem, vmem),
            scratch_shapes=[
                pltpu.SMEM(limits.shape, jnp.int32),
                pltpu.SMEM(valid_tokens.shape, jnp.int32),
                pltpu.SemaphoreType.DMA((4,)),
                pltpu.SemaphoreType.DMA,
                pltpu.SemaphoreType.DMA((n // 4,)),
                pltpu.SemaphoreType.DMA((n // 4 * 3,)),
                pltpu.SemaphoreType.DMA((n,)),
            ],
            compiler_params=pltpu.CompilerParams(collective_id=0, has_side_effects=True, vmem_limit_bytes=16 * 1024 * 1024),
            name="gather",
        )(sum_keys, sum_values, queries, limits, valid_tokens)
        return pl.pallas_call(
            attend_kernel,
            out_shape=jax.ShapeDtypeStruct((tokens, H * DV), jnp.bfloat16),
            in_specs=[vmem, vmem, vmem],
            out_specs=hbm,
            scratch_shapes=[
                pltpu.VMEM((G, 2, total, 256), jnp.bfloat16),
                pltpu.VMEM((G, 2 * total, 2 * DV), jnp.bfloat16),
                pltpu.VMEM((tokens, H * DV), jnp.bfloat16),
                pltpu.VMEM((2, tokens * (H // G // 2), total), jnp.float32),
                pltpu.VMEM((tokens * (H // G // 2), 2 * DV), jnp.float32),
                pltpu.VMEM((tokens * (H // G // 2), 2 * total), jnp.bfloat16),
                pltpu.SemaphoreType.DMA((G,)),
            ],
            compiler_params=pltpu.CompilerParams(vmem_limit_bytes=40 * 1024 * 1024),
            name="attend",
        )(q, kv, bias)

    placed = (
        P(("grp", "seq"), None),
        P(("grp", "seq"), None),
        P(("grp", "seq"), None),
        P("grp"),
        P("grp"),
    )
    return jax.shard_map(
        per_device, mesh=mesh, in_specs=placed, out_specs=P(("grp", "seq"), None), check_vma=False
    )
```

```python
import functools

import jax
import jax.numpy as jnp
from jax import lax
from jax.experimental import pallas as pl
from jax.experimental.pallas import tpu as pltpu
from jax.sharding import PartitionSpec as P

H = 64
G = 4
DK = 192
DV = 128
STRIDE = 16
CBLOCK = 32
QB = 64
LOG2E = 1.4426950408889634
MESH = pl.DeviceIdType.MESH


def gather_kernel(
    n, keys_hbm, values_hbm, q_hbm, limits_hbm, valid_ref, kv_ref, q_ref, bias_ref,
    limits_ref, in_sem, q_sem, send_sem, plane_sem, recv_sem
):
    me = lax.axis_index("seq")
    depth = n // 4
    outer = me // 4
    lane = me % 4
    kw = keys_hbm.shape[1]
    load_k = pltpu.make_async_copy(keys_hbm, kv_ref.at[me, :, pl.ds(0, kw)], in_sem.at[0])
    load_v = pltpu.make_async_copy(values_hbm, kv_ref.at[me, :, pl.ds(kw, values_hbm.shape[1])], in_sem.at[1])
    load_k.start()
    load_v.start()
    load_q = pltpu.make_async_copy(q_hbm, q_ref, q_sem)
    load_q.start()
    load_limits = pltpu.make_async_copy(limits_hbm, limits_ref, in_sem.at[2])
    load_limits.start()

    barrier = pltpu.get_barrier_semaphore()
    for step in range(1, depth):
        @pl.when(outer >= step)
        def _():
            pl.semaphore_signal(barrier, inc=1, device_id={"seq": me - 4 * step}, device_id_type=MESH)
    for step in range(1, 4):
        pl.semaphore_signal(barrier, inc=1, device_id={"seq": outer * 4 + (lane + step) % 4}, device_id_type=MESH)
    load_k.wait()
    load_v.wait()
    pl.semaphore_wait(barrier, depth - 1 - outer + 3)

    def up(step):
        return pltpu.make_async_remote_copy(
            src_ref=kv_ref.at[me],
            dst_ref=kv_ref.at[me],
            send_sem=send_sem.at[step],
            recv_sem=recv_sem.at[me],
            device_id={"seq": me + 4 * step},
            device_id_type=MESH,
        )

    def across(level, step):
        slot = level * 4 + lane
        return pltpu.make_async_remote_copy(
            src_ref=kv_ref.at[slot],
            dst_ref=kv_ref.at[slot],
            send_sem=plane_sem.at[level * 3 + step - 1],
            recv_sem=recv_sem.at[slot],
            device_id={"seq": outer * 4 + (lane + step) % 4},
            device_id_type=MESH,
        )

    def arrived(slot):
        pltpu.make_async_copy(kv_ref.at[slot], kv_ref.at[slot], recv_sem.at[slot]).wait()

    for step in range(depth - 1, 0, -1):
        @pl.when(outer + step < depth)
        def _():
            up(step).start()
    for step in range(1, 4):
        across(outer, step).start()
    load_limits.wait()
    blocks, _, total = bias_ref.shape
    usable = jnp.maximum((valid_ref[0] - CBLOCK) // STRIDE + 1, 1)
    ids = lax.broadcasted_iota(jnp.int32, (8, total), 1)
    for block in range(blocks):
        cap = jnp.minimum(limits_ref[me * blocks + block], usable)
        bias_ref[block] = jnp.where(ids < cap, 0.0, -1e30)
    for back in range(1, depth):
        @pl.when(outer >= back)
        def _():
            arrived((outer - back) * 4 + lane)
            for step in range(1, 4):
                across(outer - back, step).start()
    for level in range(depth):
        @pl.when(level > outer)
        def _():
            kv_ref[pl.ds(level * 4, 4)] = jnp.zeros((4,) + kv_ref.shape[1:], kv_ref.dtype)
    for level in range(depth):
        @pl.when(level <= outer)
        def _():
            for step in range(1, 4):
                arrived(level * 4 + (lane + step) % 4)
    for step in range(1, depth):
        @pl.when(outer + step < depth)
        def _():
            up(step).wait_send()
    for level in range(depth):
        @pl.when(level <= outer)
        def _():
            for step in range(1, 4):
                across(level, step).wait_send()
    load_q.wait()


def attend_kernel(q_ref, kv_ref, bias_ref, out_hbm, keys_ref, values_ref, out_ref, s_ref, n_ref, w_ref, out_sem):
    n, rows, _ = kv_ref.shape
    total = n * rows
    tokens = q_ref.shape[0]
    pairs = H // G // 2

    col = lax.broadcasted_iota(jnp.int32, (total, 256), 1)
    for g in range(G):
        if g % 2 == 0:
            start = g * DK
            window = kv_ref[:, :, start:start + 256].astype(jnp.float32).reshape(total, 256)
            even = jnp.where(col < DK, window, 0.0)
            odd = pltpu.roll(even, 64, 1)
        else:
            start = g * DK - 64
            window = kv_ref[:, :, start:start + 256].astype(jnp.float32).reshape(total, 256)
            odd = jnp.where(col >= 64, window, 0.0)
            even = pltpu.roll(odd, 192, 1)
        keys_ref[g, 0] = even.astype(jnp.bfloat16)
        keys_ref[g, 1] = odd.astype(jnp.bfloat16)
        start = G * DK + g * DV
        value = kv_ref[:, :, start:start + DV].astype(jnp.float32).reshape(total, DV).astype(jnp.bfloat16)
        zero = jnp.zeros((total, DV), jnp.bfloat16)
        values_ref[g, 0:total, 0:DV] = value
        values_ref[g, 0:total, DV:2 * DV] = zero
        values_ref[g, total:2 * total, 0:DV] = zero
        values_ref[g, total:2 * total, DV:2 * DV] = value

    scale = float(DK) ** -0.5 * LOG2E
    nt = (((1,), (1,)), ((), ()))
    out_cols = pairs * 2 * DV

    def put(g):
        cols = pl.ds(pl.multiple_of(g * out_cols, 128), out_cols)
        return pltpu.make_async_copy(out_ref.at[:, cols], out_hbm.at[:, cols], out_sem.at[g])

    def one_group(g, _):
        base = pl.multiple_of(g * (pairs * 2 * DK), 128)
        for half in range(2):
            q = jnp.concatenate(
                [q_ref[:, pl.ds(base + p * 2 * DK + half * 128, 256)] for p in range(pairs)], axis=0
            )
            s_ref[half] = lax.dot_general(q, keys_ref[g, half], nt, preferred_element_type=jnp.float32)
        for p in range(pairs):
            for block in range(tokens // QB):
                at = slice(p * tokens + block * QB, p * tokens + (block + 1) * QB)
                bias = bias_ref[block, 0:1, :]
                for half in range(2):
                    s = s_ref[half, at, :] + bias
                    w = jnp.exp2((s - jnp.max(s, axis=1, keepdims=True)) * scale)
                    norm = jnp.sum(w, axis=1, keepdims=True)
                    n_ref[at, half * DV:(half + 1) * DV] = jnp.broadcast_to(1.0 / norm, (QB, DV))
                    w_ref[at, half * total:(half + 1) * total] = w.astype(jnp.bfloat16)
        blended = jnp.dot(w_ref[...], values_ref[g], preferred_element_type=jnp.float32) * n_ref[...]
        for p in range(pairs):
            out_at = pl.multiple_of(g * out_cols + p * 2 * DV, 128)
            out_ref[:, pl.ds(out_at, 2 * DV)] = blended[p * tokens:(p + 1) * tokens].astype(jnp.bfloat16)
        put(g).start()
        return 0

    lax.fori_loop(0, G, one_group, 0)
    for g in range(G):
        put(g).wait()


def solution(mesh):
    n = mesh.shape["seq"]

    def per_device(queries, sum_keys, sum_values, limits, valid_tokens):
        rows = sum_keys.shape[0]
        tokens = queries.shape[0]
        width = sum_keys.shape[1] + sum_values.shape[1]
        total = n * rows
        hbm = pl.BlockSpec(memory_space=pltpu.HBM)
        vmem = pl.BlockSpec(memory_space=pltpu.VMEM)
        kv, q, bias = pl.pallas_call(
            functools.partial(gather_kernel, n),
            out_shape=(
                pltpu.VMEM((n, rows, width), jnp.bfloat16),
                pltpu.VMEM(queries.shape, jnp.bfloat16),
                pltpu.VMEM((tokens // QB, 8, total), jnp.float32),
            ),
            in_specs=[hbm, hbm, hbm, hbm, pl.BlockSpec(memory_space=pltpu.SMEM)],
            out_specs=(vmem, vmem, vmem),
            scratch_shapes=[
                pltpu.SMEM(limits.shape, jnp.int32),
                pltpu.SemaphoreType.DMA((3,)),
                pltpu.SemaphoreType.DMA,
                pltpu.SemaphoreType.DMA((n // 4,)),
                pltpu.SemaphoreType.DMA((n // 4 * 3,)),
                pltpu.SemaphoreType.DMA((n,)),
            ],
            compiler_params=pltpu.CompilerParams(collective_id=0, has_side_effects=True, vmem_limit_bytes=16 * 1024 * 1024),
            name="gather",
        )(*(
            pltpu.with_memory_space_constraint(x, pltpu.HBM)
            for x in (sum_keys, sum_values, queries, limits)
        ), valid_tokens)
        return pl.pallas_call(
            attend_kernel,
            out_shape=jax.ShapeDtypeStruct((tokens, H * DV), jnp.bfloat16),
            in_specs=[vmem, vmem, vmem],
            out_specs=hbm,
            scratch_shapes=[
                pltpu.VMEM((G, 2, total, 256), jnp.bfloat16),
                pltpu.VMEM((G, 2 * total, 2 * DV), jnp.bfloat16),
                pltpu.VMEM((tokens, H * DV), jnp.bfloat16),
                pltpu.VMEM((2, tokens * (H // G // 2), total), jnp.float32),
                pltpu.VMEM((tokens * (H // G // 2), 2 * DV), jnp.float32),
                pltpu.VMEM((tokens * (H // G // 2), 2 * total), jnp.bfloat16),
                pltpu.SemaphoreType.DMA((G,)),
            ],
            compiler_params=pltpu.CompilerParams(vmem_limit_bytes=40 * 1024 * 1024),
            name="attend",
        )(q, kv, bias)

    placed = (
        P(("grp", "seq"), None),
        P(("grp", "seq"), None),
        P(("grp", "seq"), None),
        P("grp"),
        P("grp"),
    )
    return jax.shard_map(
        per_device, mesh=mesh, in_specs=placed, out_specs=P(("grp", "seq"), None), check_vma=False
    )
```

```python
import functools

import jax
import jax.numpy as jnp
from jax import lax
from jax.experimental import pallas as pl
from jax.experimental.pallas import tpu as pltpu
from jax.sharding import PartitionSpec as P

H = 64
G = 4
DK = 192
DV = 128
STRIDE = 16
CBLOCK = 32
QB = 64
LOG2E = 1.4426950408889634
MESH = pl.DeviceIdType.MESH


def gather_kernel(
    n, keys_hbm, values_hbm, q_hbm, limits_hbm, valid_ref, kv_ref, q_ref, bias_ref,
    limits_ref, in_sem, q_sem, send_sem, plane_sem, recv_sem
):
    me = lax.axis_index("seq")
    depth = n // 4
    outer = me // 4
    lane = me % 4
    kw = keys_hbm.shape[1]
    load_k = pltpu.make_async_copy(keys_hbm, kv_ref.at[me, :, pl.ds(0, kw)], in_sem.at[0])
    load_v = pltpu.make_async_copy(values_hbm, kv_ref.at[me, :, pl.ds(kw, values_hbm.shape[1])], in_sem.at[1])
    load_k.start()
    load_v.start()
    load_q = pltpu.make_async_copy(q_hbm, q_ref, q_sem)
    load_q.start()
    load_limits = pltpu.make_async_copy(limits_hbm, limits_ref, in_sem.at[2])
    load_limits.start()

    partner = lane // 2 * 2 + (lane + 1) % 2
    near = [(lane + 2) % 4, partner]
    lanes = [lane, (lane + 2) % 4]

    barrier = pltpu.get_barrier_semaphore()
    for step in range(1, depth):
        @pl.when(outer >= step)
        def _():
            for to in lanes:
                pl.semaphore_signal(barrier, inc=1, device_id={"seq": (outer - step) * 4 + to}, device_id_type=MESH)
    for to in near:
        pl.semaphore_signal(barrier, inc=1, device_id={"seq": outer * 4 + to}, device_id_type=MESH)
    load_k.wait()
    load_v.wait()
    pl.semaphore_wait(barrier, (depth - 1 - outer) * len(lanes) + len(near))

    def push(slot, sem, target):
        return pltpu.make_async_remote_copy(
            src_ref=kv_ref.at[slot],
            dst_ref=kv_ref.at[slot],
            send_sem=sem,
            recv_sem=recv_sem.at[slot],
            device_id={"seq": target},
            device_id_type=MESH,
        )

    def up(step):
        return [
            push(me, send_sem.at[step * 4 + i], (outer + step) * 4 + to) for i, to in enumerate(lanes)
        ]

    def flat():
        return [push(me, send_sem.at[i], outer * 4 + to) for i, to in enumerate(near)]

    def arrived(slot):
        pltpu.make_async_copy(kv_ref.at[slot], kv_ref.at[slot], recv_sem.at[slot]).wait()

    for copy in flat():
        copy.start()
    for step in range(1, depth):
        @pl.when(outer + step < depth)
        def _():
            for copy in up(step):
                copy.start()
    for level in range(depth):
        @pl.when(level > outer)
        def _():
            kv_ref[pl.ds(level * 4, 4)] = jnp.zeros((4,) + kv_ref.shape[1:], kv_ref.dtype)
    load_limits.wait()
    blocks, _, total = bias_ref.shape
    usable = jnp.maximum((valid_ref[0] - CBLOCK) // STRIDE + 1, 1)
    ids = lax.broadcasted_iota(jnp.int32, (8, total), 1)
    for block in range(blocks):
        cap = jnp.minimum(limits_ref[me * blocks + block], usable)
        bias_ref[block] = jnp.where(ids < cap, 0.0, -1e30)

    def hand(slot, sem):
        return push(slot, plane_sem.at[sem], outer * 4 + partner)

    other = (lane + 2) % 4
    arrived(outer * 4 + other)
    hand(outer * 4 + other, 0).start()
    for back in range(1, depth):
        @pl.when(outer >= back)
        def _():
            for i, to in enumerate(lanes):
                arrived((outer - back) * 4 + to)
                hand((outer - back) * 4 + to, back * 2 + i).start()
    arrived(outer * 4 + partner)
    diagonal = (partner + 2) % 4
    arrived(outer * 4 + diagonal)
    hand(outer * 4 + other, 0).wait_send()
    for back in range(1, depth):
        @pl.when(outer >= back)
        def _():
            arrived((outer - back) * 4 + partner)
            arrived((outer - back) * 4 + diagonal)
            for i, to in enumerate(lanes):
                hand((outer - back) * 4 + to, back * 2 + i).wait_send()

    for copy in flat():
        copy.wait_send()
    for step in range(1, depth):
        @pl.when(outer + step < depth)
        def _():
            for copy in up(step):
                copy.wait_send()
    load_q.wait()


def attend_kernel(q_ref, kv_ref, bias_ref, out_hbm, keys_ref, values_ref, out_ref, s_ref, n_ref, w_ref, out_sem):
    n, rows, _ = kv_ref.shape
    total = n * rows
    tokens = q_ref.shape[0]
    pairs = H // G // 2

    col = lax.broadcasted_iota(jnp.int32, (total, 256), 1)
    for g in range(G):
        if g % 2 == 0:
            start = g * DK
            window = kv_ref[:, :, start:start + 256].astype(jnp.float32).reshape(total, 256)
            even = jnp.where(col < DK, window, 0.0)
            odd = pltpu.roll(even, 64, 1)
        else:
            start = g * DK - 64
            window = kv_ref[:, :, start:start + 256].astype(jnp.float32).reshape(total, 256)
            odd = jnp.where(col >= 64, window, 0.0)
            even = pltpu.roll(odd, 192, 1)
        keys_ref[g, 0] = even.astype(jnp.bfloat16)
        keys_ref[g, 1] = odd.astype(jnp.bfloat16)
        start = G * DK + g * DV
        value = kv_ref[:, :, start:start + DV].astype(jnp.float32).reshape(total, DV).astype(jnp.bfloat16)
        zero = jnp.zeros((total, DV), jnp.bfloat16)
        values_ref[g, 0:total, 0:DV] = value
        values_ref[g, 0:total, DV:2 * DV] = zero
        values_ref[g, total:2 * total, 0:DV] = zero
        values_ref[g, total:2 * total, DV:2 * DV] = value

    scale = float(DK) ** -0.5 * LOG2E
    nt = (((1,), (1,)), ((), ()))
    out_cols = pairs * 2 * DV

    def put(g):
        cols = pl.ds(pl.multiple_of(g * out_cols, 128), out_cols)
        return pltpu.make_async_copy(out_ref.at[:, cols], out_hbm.at[:, cols], out_sem.at[g])

    def one_group(g, _):
        base = pl.multiple_of(g * (pairs * 2 * DK), 128)
        for half in range(2):
            q = jnp.concatenate(
                [q_ref[:, pl.ds(base + p * 2 * DK + half * 128, 256)] for p in range(pairs)], axis=0
            )
            s_ref[half] = lax.dot_general(q, keys_ref[g, half], nt, preferred_element_type=jnp.float32)
        for p in range(pairs):
            for block in range(tokens // QB):
                at = slice(p * tokens + block * QB, p * tokens + (block + 1) * QB)
                bias = bias_ref[block, 0:1, :]
                for half in range(2):
                    s = s_ref[half, at, :] + bias
                    w = jnp.exp2((s - jnp.max(s, axis=1, keepdims=True)) * scale)
                    norm = jnp.sum(w, axis=1, keepdims=True)
                    n_ref[at, half * DV:(half + 1) * DV] = jnp.broadcast_to(1.0 / norm, (QB, DV))
                    w_ref[at, half * total:(half + 1) * total] = w.astype(jnp.bfloat16)
        for p in range(pairs):
            at = slice(p * tokens, (p + 1) * tokens)
            blended = jnp.dot(w_ref[at, :], values_ref[g], preferred_element_type=jnp.float32) * n_ref[at, :]
            out_at = pl.multiple_of(g * out_cols + p * 2 * DV, 128)
            out_ref[:, pl.ds(out_at, 2 * DV)] = blended.astype(jnp.bfloat16)
        put(g).start()
        return 0

    lax.fori_loop(0, G, one_group, 0)
    for g in range(G):
        put(g).wait()


def solution(mesh):
    n = mesh.shape["seq"]

    def per_device(queries, sum_keys, sum_values, limits, valid_tokens):
        rows = sum_keys.shape[0]
        tokens = queries.shape[0]
        width = sum_keys.shape[1] + sum_values.shape[1]
        total = n * rows
        hbm = pl.BlockSpec(memory_space=pltpu.HBM)
        vmem = pl.BlockSpec(memory_space=pltpu.VMEM)
        kv, q, bias = pl.pallas_call(
            functools.partial(gather_kernel, n),
            out_shape=(
                pltpu.VMEM((n, rows, width), jnp.bfloat16),
                pltpu.VMEM(queries.shape, jnp.bfloat16),
                pltpu.VMEM((tokens // QB, 8, total), jnp.float32),
            ),
            in_specs=[hbm, hbm, hbm, hbm, pl.BlockSpec(memory_space=pltpu.SMEM)],
            out_specs=(vmem, vmem, vmem),
            scratch_shapes=[
                pltpu.SMEM(limits.shape, jnp.int32),
                pltpu.SemaphoreType.DMA((3,)),
                pltpu.SemaphoreType.DMA,
                pltpu.SemaphoreType.DMA((n,)),
                pltpu.SemaphoreType.DMA((n // 4 * 3,)),
                pltpu.SemaphoreType.DMA((n,)),
            ],
            compiler_params=pltpu.CompilerParams(collective_id=0, has_side_effects=True, vmem_limit_bytes=16 * 1024 * 1024),
            name="gather",
        )(*(
            pltpu.with_memory_space_constraint(x, pltpu.HBM)
            for x in (sum_keys, sum_values, queries, limits)
        ), valid_tokens)
        return pl.pallas_call(
            attend_kernel,
            out_shape=jax.ShapeDtypeStruct((tokens, H * DV), jnp.bfloat16),
            in_specs=[vmem, vmem, vmem],
            out_specs=hbm,
            scratch_shapes=[
                pltpu.VMEM((G, 2, total, 256), jnp.bfloat16),
                pltpu.VMEM((G, 2 * total, 2 * DV), jnp.bfloat16),
                pltpu.VMEM((tokens, H * DV), jnp.bfloat16),
                pltpu.VMEM((2, tokens * (H // G // 2), total), jnp.float32),
                pltpu.VMEM((tokens * (H // G // 2), 2 * DV), jnp.float32),
                pltpu.VMEM((tokens * (H // G // 2), 2 * total), jnp.bfloat16),
                pltpu.SemaphoreType.DMA((G,)),
            ],
            compiler_params=pltpu.CompilerParams(vmem_limit_bytes=40 * 1024 * 1024),
            name="attend",
        )(q, kv, bias)

    placed = (
        P(("grp", "seq"), None),
        P(("grp", "seq"), None),
        P(("grp", "seq"), None),
        P("grp"),
        P("grp"),
    )
    return jax.shard_map(
        per_device, mesh=mesh, in_specs=placed, out_specs=P(("grp", "seq"), None), check_vma=False
    )
```
